32 devices in a mesh: groups: 2 (over y), blk: 16 (over z, x, core).
Axes of the slice: x: 2, y: 2, z: 4, core: 2. Of those that a mesh axis runs over, the one named last changes fastest.
Arguments:
- current_states: float32 [16, 8192], P(None, ('groups', 'blk')), parts along dimension 1, may hold values from -0.5 to 0.5
- next_states: float32 [16, 8192], P(None, ('groups', 'blk')), parts along dimension 1, may hold values from -1 to 1
- next_values: float32 [8192], P(('groups', 'blk')), parts along dimension 0, may hold values from 0 to 2.5
- vol_table: float32 [12, 16], replicated, may hold values from 0.15 to 0.45
- date_index: int32 [1], replicated, may hold values from 0 to 11
- strike: float32 [1], replicated, may hold values from 0.8 to 1.2
Outputs:
- continuation: float32 [8192], P(('groups', 'blk')), parts along dimension 0
- node_value: float32 [8192], P(('groups', 'blk')), parts along dimension 0
The draws below stay inside these ranges and needn't reach their ends.
There are 2 independent parts, one for each index of `groups`. The reference program is written for one: setup_inputs(seed, part) draws one part's arguments, and reference() takes and returns one part's arrays. A program takes and returns all parts, laid end to end along the dimension named above; an argument that names none is the same for every part. Nothing has to cross between parts.
All inputs are finite; a program needn't handle non-finite values.
Results may differ from the reference program's by a relative error of at most 0.00012.
Values sent between devices are 32-bit elements; how exact they have to be, the bound alone decides.
No kernel may reach another device: no remote copies, remote signals or barrier semaphores. Data moves between devices by JAX's collectives and lax.ppermute only.
A program may use at most 64 MiB of HBM per device.

```python
import math
import jax
import jax.numpy as jnp
from jax import lax

ASSETS = 16
DATES = 12
NODES = 4096


def mesh_paths(key):
    folded = jax.random.fold_in(key, 7)
    key_list = jax.random.split(folded, 5)
    placing = (jnp.arange(NODES, dtype=jnp.float32) + 0.5) / NODES - 0.5
    heading = 0.05 * jnp.clip(jax.random.normal(key_list[0], (ASSETS,), jnp.float32), -2.0, 2.0)
    widths = jnp.exp(jax.random.uniform(key_list[1], (ASSETS,), jnp.float32, jnp.log(0.5), jnp.log(1.5)))
    jitter = jnp.clip(jax.random.normal(key_list[2], (ASSETS, NODES), jnp.float32), -4.0, 4.0)
    current = 0.03 * widths[:, None] * jitter + heading[:, None] * placing[None, :]
    moves = jnp.clip(jax.random.normal(key_list[3], (ASSETS, NODES), jnp.float32), -4.0, 4.0)
    following = current - 0.004 + 0.095 * moves
    extra = jnp.clip(jax.random.normal(key_list[4], (NODES,), jnp.float32), -4.0, 4.0)
    worth = jnp.maximum(jnp.max(jnp.exp(following), axis=0) - 1.0, 0.0) + 0.05 * jnp.exp(0.5 * extra)
    return (current, following, worth)


def draw_current_states(key, part):
    return mesh_paths(key)[0]


def draw_next_states(key, part):
    return mesh_paths(key)[1]


def draw_next_values(key, part):
    return mesh_paths(key)[2]


def setup_inputs(seed: int = 0, part: int = 0) -> dict:
    keys = jax.random.split(jax.random.key(seed), 7)
    own_keys = jax.random.split(jax.random.fold_in(keys[6], part), 7)
    return {
        "current_states": draw_current_states(jax.random.fold_in(jax.random.fold_in(keys[6], part), 71), part),
        "next_states": draw_next_states(jax.random.fold_in(jax.random.fold_in(keys[6], part), 71), part),
        "next_values": draw_next_values(jax.random.fold_in(jax.random.fold_in(keys[6], part), 71), part),
        "vol_table": jnp.clip(jnp.exp(jax.random.uniform(keys[3], (DATES, ASSETS), jnp.float32, math.log(0.15), math.log(0.45))), 0.15, 0.45),
        "date_index": jax.random.randint(keys[4], (1,), 0, DATES).astype(jnp.int32),
        "strike": jnp.clip(jax.random.uniform(keys[5], (1,), jnp.float32, 0.8, 1.2), 0.8, 1.2),
    }


rate_year = 0.05
step_years = 0.1

def scaled_states(current_states, next_states, vol_table, date_index):
    date_count = vol_table.shape[0]
    picked = (jnp.arange(date_count, dtype=jnp.int32) == date_index[0]).astype(jnp.float32)
    vol_row = lax.optimization_barrier(jnp.sum(vol_table * picked[:, None], axis=0))
    spread = vol_row * math.sqrt(step_years)
    drift_term = (rate_year - 0.5 * vol_row * vol_row) * step_years
    anchor = (current_states + drift_term[:, None]) / spread[:, None]
    target = next_states / spread[:, None]
    anchor_half = 0.5 * lax.optimization_barrier(jnp.sum(anchor * anchor, axis=0, keepdims=True))
    target_half = 0.5 * lax.optimization_barrier(jnp.sum(target * target, axis=0, keepdims=True))
    return (anchor, anchor_half, target, target_half)

def kernel_block(source_states, source_norms, sink_states, sink_norms):
    inner_term = lax.dot_general(source_states, sink_states, (((0,), (0,)), ((), ())), precision=lax.Precision.HIGHEST, preferred_element_type=jnp.float32)
    return jnp.exp(inner_term - source_norms.reshape(-1, 1) - sink_norms.reshape(1, -1))

def finish(current_states, totals, strike):
    continuation = math.exp(-rate_year * step_years) * totals[0] / totals[1]
    payoff = jnp.maximum(lax.optimization_barrier(jnp.max(jnp.exp(current_states), axis=0)) - strike[0], 0.0)
    return (continuation, jnp.maximum(payoff, continuation))

def reference(current_states, next_states, next_values, vol_table, date_index, strike):
    anchor, anchor_half, target, target_half = scaled_states(current_states, next_states, vol_table, date_index)
    node_count = anchor.shape[1]
    block_size = math.gcd(node_count, 1024)
    blocks = node_count // block_size

    def density_block(number):
        sink_part = lax.dynamic_slice_in_dim(target, number * block_size, block_size, 1)
        norm_part = lax.dynamic_slice_in_dim(target_half, number * block_size, block_size, 1)
        return lax.optimization_barrier(jnp.sum(kernel_block(sink_part, norm_part, anchor, anchor_half), axis=1))
    density = lax.map(density_block, jnp.arange(blocks, dtype=jnp.int32)).reshape(-1)
    ratios = jnp.stack([next_values / density, 1.0 / density], axis=0)

    def weighted_block(number):
        anchor_part = lax.dynamic_slice_in_dim(anchor, number * block_size, block_size, 1)
        half_part = lax.dynamic_slice_in_dim(anchor_half, number * block_size, block_size, 1)
        weights = kernel_block(target, target_half, anchor_part, half_part)
        return jnp.dot(ratios, weights, precision=lax.Precision.HIGHEST, preferred_element_type=jnp.float32)
    totals = lax.map(weighted_block, jnp.arange(blocks, dtype=jnp.int32))
    totals = jnp.transpose(totals, (1, 0, 2)).reshape(2, -1)
    return finish(current_states, totals, strike)
```

```python
import functools
import math

import jax
import jax.numpy as jnp
from jax import lax
from jax.experimental import pallas as pl
from jax.experimental.pallas import tpu as pltpu
from jax.sharding import PartitionSpec as P

rate_year = 0.05
step_years = 0.1
log2_e = math.log2(math.e)
lane_tile = 512
row_tile = 256
depth = 128
doubling_limit = 32


def scaled_states(current_states, next_states, vol_table, date_index):
    date_count = vol_table.shape[0]
    picked = (jnp.arange(date_count, dtype=jnp.int32) == date_index[0]).astype(jnp.float32)
    vol_row = jnp.sum(vol_table * picked[:, None], axis=0)
    spread = vol_row * math.sqrt(step_years)
    drift_term = (rate_year - 0.5 * vol_row * vol_row) * step_years
    anchor = (current_states + drift_term[:, None]) / spread[:, None]
    target = next_states / spread[:, None]
    anchor_half = 0.5 * jnp.sum(anchor * anchor, axis=0, keepdims=True)
    target_half = 0.5 * jnp.sum(target * target, axis=0, keepdims=True)
    return (anchor, anchor_half, target, target_half)


def kernel_block(source_states, source_norms, sink_states, sink_norms):
    inner_term = lax.dot_general(
        source_states,
        sink_states,
        (((0,), (0,)), ((), ())),
        precision=lax.Precision.HIGHEST,
        preferred_element_type=jnp.float32,
    )
    return jnp.exp(inner_term - source_norms.reshape(-1, 1) - sink_norms)


def block_rows(row_count):
    if row_count <= 4096:
        return row_count
    return math.gcd(row_count, 4096)


def finish(current_states, totals, strike):
    continuation = math.exp(-rate_year * step_years) * totals[0] / totals[1]
    payoff = jnp.maximum(jnp.max(jnp.exp(current_states), axis=0) - strike[0], 0.0)
    return (continuation, jnp.maximum(payoff, continuation))


def gathered_body(current_states, next_states, next_values, vol_table, date_index, strike):
    anchor, anchor_half, target, target_half = scaled_states(
        current_states, next_states, vol_table, date_index
    )
    local_count = anchor.shape[1]
    pieces = (
        lax.all_gather(anchor, "blk", axis=1, tiled=True),
        lax.all_gather(anchor_half, "blk", axis=1, tiled=True),
    )
    row_count = pieces[0].shape[1]
    block_size = block_rows(row_count)

    def density_block(number, inner_sum):
        source_part = lax.dynamic_slice_in_dim(pieces[0], number * block_size, block_size, 1)
        norm_part = lax.dynamic_slice_in_dim(pieces[1], number * block_size, block_size, 1)
        return inner_sum + jnp.sum(
            kernel_block(source_part, norm_part, target, target_half), axis=0
        )

    density = lax.fori_loop(
        0, row_count // block_size, density_block, jnp.zeros((local_count,), jnp.float32)
    )
    extras = jnp.concatenate(
        [target_half, (next_values / density)[None, :], (1.0 / density)[None, :]], axis=0
    )
    add_pieces = (
        lax.all_gather(target, "blk", axis=1, tiled=True),
        lax.all_gather(extras, "blk", axis=1, tiled=True),
    )

    def weighted_block(number, inner_sum):
        sink_part = lax.dynamic_slice_in_dim(add_pieces[0], number * block_size, block_size, 1)
        extra_part = lax.dynamic_slice_in_dim(add_pieces[1], number * block_size, block_size, 1)
        weights = kernel_block(sink_part, extra_part[0:1], anchor, anchor_half)
        return inner_sum + jnp.dot(
            extra_part[1:3],
            weights,
            precision=lax.Precision.HIGHEST,
            preferred_element_type=jnp.float32,
        )

    totals = lax.fori_loop(
        0, row_count // block_size, weighted_block, jnp.zeros((2, local_count), jnp.float32)
    )
    return finish(current_states, totals, strike)


def spread_columns(vol_ref, index_ref):
    dates, assets = vol_ref.shape
    rows = lax.broadcasted_iota(jnp.int32, (dates, assets), 0)
    vol_row = jnp.sum(jnp.where(rows == index_ref[0], vol_ref[...], 0.0), axis=0, keepdims=True)
    square = (assets, assets)
    diagonal = lax.broadcasted_iota(jnp.int32, square, 0) == lax.broadcasted_iota(
        jnp.int32, square, 1
    )
    vol = jnp.sum(
        jnp.where(diagonal, jnp.broadcast_to(vol_row, square), 0.0), axis=1, keepdims=True
    )
    spread = vol * math.sqrt(step_years)
    drift_term = (rate_year - 0.5 * vol * vol) * step_years
    return 1.0 / spread, drift_term


def in_three(x):
    first = x.astype(jnp.bfloat16)
    rest = x - first.astype(jnp.float32)
    second = rest.astype(jnp.bfloat16)
    third = (rest - second.astype(jnp.float32)).astype(jnp.bfloat16)
    return first, second, third


def with_norm(pieces, norm, ones_first):
    rows = lax.broadcasted_iota(jnp.int32, (16, norm.shape[1]), 0)
    shift = 3 if ones_first else 0
    tile = jnp.where((rows >= 3 - shift) & (rows < 6 - shift), 1.0, 0.0)
    for k, part in enumerate(in_three(norm)):
        tile = jnp.where(rows == k + shift, part.astype(jnp.float32), tile)
    return jnp.concatenate(list(pieces) + [tile.astype(jnp.bfloat16)], axis=0)


def source_operand(states, inverse, drift_term):
    anchor = (states + drift_term) * inverse
    half = (0.5 * log2_e) * jnp.sum(anchor * anchor, axis=0, keepdims=True)
    a1, a2, a3 = in_three(anchor * log2_e)
    stacked = with_norm((a1, a1, a2, a1, a2, a3), -half, False)
    fill = jnp.zeros((depth - stacked.shape[0], stacked.shape[1]), jnp.bfloat16)
    return jnp.concatenate([stacked, fill], axis=0).T


def sink_operand(states, inverse):
    target = states * inverse
    half = (0.5 * log2_e) * jnp.sum(target * target, axis=0, keepdims=True)
    t1, t2, t3 = in_three(target)
    stacked = with_norm((t1, t2, t1, t3, t2, t1), -half, True)
    fill = jnp.zeros((depth - stacked.shape[0], stacked.shape[1]), jnp.bfloat16)
    return jnp.concatenate([stacked, fill], axis=0)


def partial_density(left_ref, right_ref, density_ref):
    source_count, sink_count = left_ref.shape[0], right_ref.shape[1]
    width = math.gcd(sink_count, lane_tile)
    height = math.gcd(source_count, row_tile)

    def columns(number, carry):
        part = pl.ds(pl.multiple_of(number * width, width), width)
        right = right_ref[:, part]
        total = jnp.zeros((8, width), jnp.float32)
        for k in range(source_count // height):
            exponent = jnp.dot(
                left_ref[k * height : (k + 1) * height, :],
                right,
                preferred_element_type=jnp.float32,
            )
            total += jnp.sum(jnp.exp2(exponent).reshape(height // 8, 8, width), axis=0)
        density_ref[:, part] = jnp.sum(total, axis=0, keepdims=True)
        return carry

    lax.fori_loop(0, sink_count // width, columns, 0)


def own_kernel(assets, index_ref, vol_ref, blocks_ref, left_ref, right_ref, density_ref):
    inverse, drift_term = spread_columns(vol_ref, index_ref)
    count = blocks_ref.shape[2]
    for b in range(blocks_ref.shape[0]):
        part = slice(b * count, (b + 1) * count)
        left_ref[part, :] = source_operand(blocks_ref[b, 0:assets, :], inverse, drift_term)
        right_ref[:, part] = sink_operand(blocks_ref[b, assets : 2 * assets, :], inverse)
    partial_density(left_ref, right_ref, density_ref)


def other_kernel(assets, index_ref, vol_ref, blocks_ref, left_ref, right_ref, density_ref):
    inverse, _ = spread_columns(vol_ref, index_ref)
    count = blocks_ref.shape[2]
    for b in range(blocks_ref.shape[0]):
        part = slice(b * count, (b + 1) * count)
        right_ref[:, part] = sink_operand(blocks_ref[b, 0:assets, :], inverse)
    partial_density(left_ref, right_ref, density_ref)


def weight_kernel(
    assets,
    strike_ref,
    blocks_ref,
    others_ref,
    left_ref,
    right_ref,
    other_right_ref,
    density_ref,
    received_ref,
    continuation_ref,
    node_ref,
    ratio_ref,
):
    block_count, _, count = blocks_ref.shape
    half = block_count * count
    for k, (values_ref, row) in enumerate(((blocks_ref, 2 * assets), (others_ref, assets))):
        inverse = 1.0 / (density_ref[k : k + 1, :] + received_ref[1 - k : 2 - k, :])
        ratio_ref[1:2, k * half : (k + 1) * half] = inverse
        for b in range(block_count):
            part = slice(b * count, (b + 1) * count)
            ratio_ref[0:1, k * half + b * count : k * half + (b + 1) * count] = (
                values_ref[b, row : row + 1, :] * inverse[:, part]
            )
    width = math.gcd(half, lane_tile)
    left = left_ref[...]
    weighted = jnp.zeros((count, 128), jnp.float32)
    mass = jnp.zeros((count, 128), jnp.float32)
    for k, operand_ref in enumerate((right_ref, other_right_ref)):
        for number in range(half // width):
            weights = jnp.exp2(
                jnp.dot(
                    left,
                    operand_ref[:, number * width : (number + 1) * width],
                    preferred_element_type=jnp.float32,
                )
            )
            for lane in range(0, width, 128):
                place = k * half + number * width + lane
                piece = weights[:, lane : lane + 128]
                weighted += piece * ratio_ref[0:1, place : place + 128]
                mass += piece * ratio_ref[1:2, place : place + 128]
    weighted_row = jnp.sum(weighted.T, axis=0, keepdims=True)
    mass_row = jnp.sum(mass.T, axis=0, keepdims=True)
    continuation = math.exp(-rate_year * step_years) * weighted_row / mass_row
    best = jnp.max(jnp.exp(blocks_ref[0, 0:assets, :]), axis=0, keepdims=True)
    payoff = jnp.maximum(best - strike_ref[0], 0.0)
    continuation_ref[...] = continuation
    node_ref[...] = jnp.maximum(payoff, continuation)


smem = pl.BlockSpec(memory_space=pltpu.SMEM)
vmem = pl.BlockSpec(memory_space=pltpu.VMEM)


def doubled_body(blk_size, current_states, next_states, next_values, vol_table, date_index, strike):
    assets, count = current_states.shape

    def across(array, mask):
        return lax.ppermute(array, "blk", [(i, i ^ mask) for i in range(blk_size)])

    blocks = jnp.concatenate([current_states, next_states, next_values[None, :]], axis=0)[None]
    mask = blk_size // 2
    while mask > 1:
        blocks = jnp.concatenate([blocks, across(blocks, mask)], axis=0)
        mask //= 2
    others = across(blocks[:, assets:, :], 1)
    half = blocks.shape[0] * count
    left_shape = jax.ShapeDtypeStruct((half, depth), jnp.bfloat16)
    right_shape = jax.ShapeDtypeStruct((depth, half), jnp.bfloat16)
    density_shape = jax.ShapeDtypeStruct((1, half), jnp.float32)
    cost = pl.CostEstimate(
        flops=2 * depth * half * half, transcendentals=half * half, bytes_accessed=0
    )
    left, right, own_density = pl.pallas_call(
        functools.partial(own_kernel, assets),
        out_shape=(left_shape, right_shape, density_shape),
        in_specs=[smem, vmem, vmem],
        out_specs=(vmem, vmem, vmem),
        cost_estimate=cost,
        name="own_density",
    )(date_index, vol_table, blocks)
    other_right, other_density = pl.pallas_call(
        functools.partial(other_kernel, assets),
        out_shape=(right_shape, density_shape),
        in_specs=[smem, vmem, vmem, vmem],
        out_specs=(vmem, vmem),
        cost_estimate=cost,
        name="other_density",
    )(date_index, vol_table, others, left)
    density = jnp.concatenate([own_density, other_density], axis=0)
    received = across(density, 1)
    row_shape = jax.ShapeDtypeStruct((1, count), jnp.float32)
    continuation, node_value = pl.pallas_call(
        functools.partial(weight_kernel, assets),
        grid=(1,),
        out_shape=(row_shape, row_shape),
        in_specs=[smem, vmem, vmem, pl.BlockSpec((count, depth), lambda i: (0, 0)), vmem, vmem, vmem, vmem],
        out_specs=(vmem, vmem),
        scratch_shapes=[pltpu.VMEM((2, 2 * half), jnp.float32)],
        name="weights",
    )(strike, blocks, others, left, right, other_right, density, received)
    return continuation.reshape(count), node_value.reshape(count)


def solution(mesh):
    blk_size = mesh.shape["blk"]
    placed = (
        P(None, ("groups", "blk")),
        P(None, ("groups", "blk")),
        P(("groups", "blk")),
        P(),
        P(),
        P(),
    )
    doubled = 2 <= blk_size <= doubling_limit and blk_size & (blk_size - 1) == 0
    return jax.shard_map(
        functools.partial(doubled_body, blk_size) if doubled else gathered_body,
        mesh=mesh,
        in_specs=placed,
        out_specs=(P(("groups", "blk")), P(("groups", "blk"))),
        check_vma=False,
    )
```

```python
import functools
import math

import jax
import jax.numpy as jnp
from jax import lax
from jax.experimental import pallas as pl
from jax.experimental.pallas import tpu as pltpu
from jax.sharding import PartitionSpec as P

rate_year = 0.05
step_years = 0.1
log2_e = math.log2(math.e)
lanes = 128
lane_tile = 512
row_tile = 256
depth = 128
vmem_grant = 16 * 1024 * 1024


def scaled_states(current_states, next_states, vol_table, date_index):
    date_count = vol_table.shape[0]
    picked = (jnp.arange(date_count, dtype=jnp.int32) == date_index[0]).astype(jnp.float32)
    vol_row = jnp.sum(vol_table * picked[:, None], axis=0)
    spread = vol_row * math.sqrt(step_years)
    drift_term = (rate_year - 0.5 * vol_row * vol_row) * step_years
    anchor = (current_states + drift_term[:, None]) / spread[:, None]
    target = next_states / spread[:, None]
    anchor_half = 0.5 * jnp.sum(anchor * anchor, axis=0, keepdims=True)
    target_half = 0.5 * jnp.sum(target * target, axis=0, keepdims=True)
    return (anchor, anchor_half, target, target_half)


def kernel_block(source_states, source_norms, sink_states, sink_norms):
    inner_term = lax.dot_general(
        source_states,
        sink_states,
        (((0,), (0,)), ((), ())),
        precision=lax.Precision.HIGHEST,
        preferred_element_type=jnp.float32,
    )
    return jnp.exp(inner_term - source_norms.reshape(-1, 1) - sink_norms)


def block_rows(row_count):
    if row_count <= 4096:
        return row_count
    return math.gcd(row_count, 4096)


def finish(current_states, totals, strike):
    continuation = math.exp(-rate_year * step_years) * totals[0] / totals[1]
    payoff = jnp.maximum(jnp.max(jnp.exp(current_states), axis=0) - strike[0], 0.0)
    return (continuation, jnp.maximum(payoff, continuation))


def gathered_body(current_states, next_states, next_values, vol_table, date_index, strike):
    anchor, anchor_half, target, target_half = scaled_states(
        current_states, next_states, vol_table, date_index
    )
    local_count = anchor.shape[1]
    pieces = (
        lax.all_gather(anchor, "blk", axis=1, tiled=True),
        lax.all_gather(anchor_half, "blk", axis=1, tiled=True),
    )
    row_count = pieces[0].shape[1]
    block_size = block_rows(row_count)

    def density_block(number, inner_sum):
        source_part = lax.dynamic_slice_in_dim(pieces[0], number * block_size, block_size, 1)
        norm_part = lax.dynamic_slice_in_dim(pieces[1], number * block_size, block_size, 1)
        return inner_sum + jnp.sum(
            kernel_block(source_part, norm_part, target, target_half), axis=0
        )

    density = lax.fori_loop(
        0, row_count // block_size, density_block, jnp.zeros((local_count,), jnp.float32)
    )
    extras = jnp.concatenate(
        [target_half, (next_values / density)[None, :], (1.0 / density)[None, :]], axis=0
    )
    add_pieces = (
        lax.all_gather(target, "blk", axis=1, tiled=True),
        lax.all_gather(extras, "blk", axis=1, tiled=True),
    )

    def weighted_block(number, inner_sum):
        sink_part = lax.dynamic_slice_in_dim(add_pieces[0], number * block_size, block_size, 1)
        extra_part = lax.dynamic_slice_in_dim(add_pieces[1], number * block_size, block_size, 1)
        weights = kernel_block(sink_part, extra_part[0:1], anchor, anchor_half)
        return inner_sum + jnp.dot(
            extra_part[1:3],
            weights,
            precision=lax.Precision.HIGHEST,
            preferred_element_type=jnp.float32,
        )

    totals = lax.fori_loop(
        0, row_count // block_size, weighted_block, jnp.zeros((2, local_count), jnp.float32)
    )
    return finish(current_states, totals, strike)


def in_three(x):
    first = x.astype(jnp.bfloat16)
    rest = x - first.astype(jnp.float32)
    second = rest.astype(jnp.bfloat16)
    third = (rest - second.astype(jnp.float32)).astype(jnp.bfloat16)
    return first, second, third


def with_norm(pieces, norm, shift):
    rows = lax.broadcasted_iota(jnp.int32, (16, norm.shape[1]), 0)
    tile = jnp.where((rows >= 3 - shift) & (rows < 6 - shift), 1.0, 0.0)
    for k, part in enumerate(in_three(norm)):
        tile = jnp.where(rows == k + shift, part.astype(jnp.float32), tile)
    stacked = list(pieces) + [tile.astype(jnp.bfloat16)]
    height = sum(piece.shape[0] for piece in stacked)
    stacked.append(jnp.zeros((depth - height, norm.shape[1]), jnp.bfloat16))
    return jnp.concatenate(stacked, axis=0)


def source_operand(states, inverse, drift_term):
    anchor = (states + drift_term) * inverse
    half = (0.5 * log2_e) * jnp.sum(anchor * anchor, axis=0, keepdims=True)
    a1, a2, a3 = in_three(anchor * log2_e)
    return with_norm((a1, a1, a2, a1, a2, a3), -half, 0).T


def sink_operand(states, inverse):
    target = states * inverse
    half = (0.5 * log2_e) * jnp.sum(target * target, axis=0, keepdims=True)
    t1, t2, t3 = in_three(target)
    return with_norm((t1, t2, t1, t3, t2, t1), -half, 3)


def build_sources(states_ref, columns_ref, left_ref):
    inverse, drift_term = columns_ref[0], columns_ref[1]
    assets = inverse.shape[0]
    for slab in range(left_ref.shape[0] // lanes):
        states = states_ref[slab * assets : (slab + 1) * assets, :]
        left_ref[slab * lanes : (slab + 1) * lanes, :] = source_operand(states, inverse, drift_term)


def build_sinks(states_ref, start, columns_ref, right_ref):
    inverse = columns_ref[0]
    assets = inverse.shape[0]
    for slab in range(right_ref.shape[1] // lanes):
        states = states_ref[start + slab * assets : start + (slab + 1) * assets, :]
        right_ref[:, slab * lanes : (slab + 1) * lanes] = sink_operand(states, inverse)


def add_density(left_refs, right_ref, density_ref, first_row, base_ref):
    width = math.gcd(right_ref.shape[1], lane_tile)
    for number in range(right_ref.shape[1] // width):
        right = right_ref[:, number * width : (number + 1) * width]
        total = jnp.zeros((8, width), jnp.float32)
        for left_ref in left_refs:
            height = math.gcd(left_ref.shape[0], row_tile)
            for k in range(left_ref.shape[0] // height):
                exponent = jnp.dot(
                    left_ref[k * height : (k + 1) * height, :],
                    right,
                    preferred_element_type=jnp.float32,
                )
                total += jnp.sum(jnp.exp2(exponent).reshape(height // 8, 8, width), axis=0)
        sums = jnp.sum(total, axis=0, keepdims=True)
        for slab in range(width // lanes):
            row = number * (width // lanes) + slab
            value = sums[:, slab * lanes : (slab + 1) * lanes]
            if base_ref is not None:
                value += base_ref[row : row + 1, :]
            density_ref[first_row + row : first_row + row + 1, :] = value


def pack_kernel(*refs):
    row = 0
    for ref in refs[:-1]:
        height = min(ref.shape[0], refs[-1].shape[0] - row)
        refs[-1][row : row + height, :] = ref[0:height, :]
        row += height


def side_kernel(table_ref, packed_ref, columns_ref, payoff_ref):
    dates, assets = table_ref.shape[0] - 1, table_ref.shape[1]
    index = table_ref[dates : dates + 1, 0:1]
    strike = table_ref[dates : dates + 1, 1:2]
    rows = lax.broadcasted_iota(jnp.int32, (dates, assets), 0).astype(jnp.float32)
    vol_row = jnp.sum(
        jnp.where(rows == index, table_ref[0:dates, :], 0.0), axis=0, keepdims=True
    )
    square = (assets, assets)
    diagonal = lax.broadcasted_iota(jnp.int32, square, 0) == lax.broadcasted_iota(
        jnp.int32, square, 1
    )
    vol = jnp.sum(
        jnp.where(diagonal, jnp.broadcast_to(vol_row, square), 0.0), axis=1, keepdims=True
    )
    vol = jnp.broadcast_to(vol, (assets, lanes))
    columns_ref[0] = 1.0 / (vol * math.sqrt(step_years))
    columns_ref[1] = (rate_year - 0.5 * vol * vol) * step_years
    for slab in range(payoff_ref.shape[0]):
        prices = jnp.exp(packed_ref[slab * assets : (slab + 1) * assets, :])
        best = jnp.max(prices, axis=0, keepdims=True)
        payoff_ref[slab : slab + 1, :] = jnp.maximum(best - strike, 0.0)


def column_kernel(sources, columns_ref, packed_ref, left_ref, right_ref, density_ref):
    build_sources(packed_ref, columns_ref, left_ref)
    build_sinks(packed_ref, sources, columns_ref, right_ref)
    add_density((left_ref,), right_ref, density_ref, 0, None)


def column_other_kernel(columns_ref, other_ref, left_ref, right_ref, density_ref):
    build_sinks(other_ref, 0, columns_ref, right_ref)
    add_density((left_ref,), right_ref, density_ref, 0, None)


def far_kernel(
    sources,
    columns_ref,
    packed_ref,
    left_ref,
    right_ref,
    base_ref,
    far_left_ref,
    far_right_ref,
    density_ref,
):
    build_sources(packed_ref, columns_ref, far_left_ref)
    build_sinks(packed_ref, sources, columns_ref, far_right_ref)
    add_density((far_left_ref,), right_ref, density_ref, 0, base_ref)
    add_density((left_ref, far_left_ref), far_right_ref, density_ref, base_ref.shape[0], None)


def far_other_kernel(
    columns_ref,
    other_ref,
    left_ref,
    far_left_ref,
    right_ref,
    base_ref,
    far_right_ref,
    density_ref,
):
    build_sinks(other_ref, 0, columns_ref, far_right_ref)
    add_density((far_left_ref,), right_ref, density_ref, 0, base_ref)
    add_density((left_ref, far_left_ref), far_right_ref, density_ref, base_ref.shape[0], None)


def matrix_kernel(left_ref, *refs):
    matrix_ref = refs[-1]
    place = 0
    for right_ref in refs[:-1]:
        width = math.gcd(right_ref.shape[1], lane_tile)
        for number in range(right_ref.shape[1] // width):
            matrix_ref[:, place : place + width] = jnp.exp2(
                jnp.dot(
                    left_ref[...],
                    right_ref[:, number * width : (number + 1) * width],
                    preferred_element_type=jnp.float32,
                )
            )
            place += width


def weight_kernel(
    values_start,
    matrix_ref,
    density_ref,
    received_ref,
    packed_ref,
    far_packed_ref,
    other_ref,
    far_other_ref,
    payoff_ref,
    continuation_ref,
    node_ref,
    ratio_ref,
):
    slabs = density_ref.shape[0]
    half = slabs // 2
    quarter = half // 2
    inverse = 1.0 / jnp.concatenate(
        [
            density_ref[:half, :] + received_ref[half:, :],
            density_ref[half:, :] + received_ref[:half, :],
        ],
        axis=0,
    )
    ratio_ref[1] = inverse
    other_start = other_ref.shape[0] - quarter
    for k, (values_ref, start) in enumerate(
        (
            (packed_ref, values_start),
            (far_packed_ref, values_start),
            (other_ref, other_start),
            (far_other_ref, other_start),
        )
    ):
        part = slice(k * quarter, (k + 1) * quarter)
        ratio_ref[0, part, :] = values_ref[start : start + quarter, :] * inverse[part]
    count = matrix_ref.shape[0]
    height = math.gcd(count, 64)
    sums = []
    for k in range(count // height):
        weighted = jnp.zeros((height, lanes), jnp.float32)
        mass = jnp.zeros((height, lanes), jnp.float32)
        for slab in range(slabs):
            piece = matrix_ref[k * height : (k + 1) * height, slab * lanes : (slab + 1) * lanes]
            weighted += piece * ratio_ref[0, slab : slab + 1, :]
            mass += piece * ratio_ref[1, slab : slab + 1, :]
        sums.append((weighted, mass))
    per_slab = lanes // height
    for slab in range(count // lanes):
        group = sums[slab * per_slab : (slab + 1) * per_slab]
        weighted, mass = (
            jnp.sum(jnp.concatenate([pair[k] for pair in group], axis=0).T, axis=0, keepdims=True)
            for k in range(2)
        )
        continuation = math.exp(-rate_year * step_years) * weighted / mass
        continuation_ref[slab : slab + 1, :] = continuation
        node_ref[slab : slab + 1, :] = jnp.maximum(payoff_ref[slab : slab + 1, :], continuation)


vmem = pl.BlockSpec(memory_space=pltpu.VMEM)


def local_call(kernel, name, in_specs, out_shapes, matmul_pairs=0, scratch_shapes=()):
    cost = pl.CostEstimate(
        flops=2 * depth * matmul_pairs, transcendentals=matmul_pairs, bytes_accessed=0
    )
    return pl.pallas_call(
        kernel,
        out_shape=out_shapes,
        in_specs=in_specs,
        out_specs=[vmem] * len(out_shapes),
        scratch_shapes=scratch_shapes,
        cost_estimate=cost,
        compiler_params=pltpu.CompilerParams(vmem_limit_bytes=vmem_grant),
        name=name,
    )


def doubled_body(blk_size, current_states, next_states, next_values, vol_table, date_index, strike):
    assets, count = current_states.shape
    own_slabs = count // lanes

    def across(array, mask):
        return lax.ppermute(array, "blk", [(i, i ^ mask) for i in range(blk_size)])

    def floats(*shape):
        return jax.ShapeDtypeStruct(shape, jnp.float32)

    def halves(*shape):
        return jax.ShapeDtypeStruct(shape, jnp.bfloat16)

    pieces = [
        part[:, slab * lanes : (slab + 1) * lanes]
        for part in (current_states, next_states)
        for slab in range(own_slabs)
    ]
    rows = lax.pad(
        next_values.reshape(own_slabs, lanes), jnp.float32(0), ((0, assets - own_slabs, 0), (0, 0, 0))
    )
    tile_rows = lax.broadcasted_iota(jnp.int32, rows.shape, 0)
    pieces.append(jnp.where(tile_rows < own_slabs, rows, pieces[0]))
    (packed,) = local_call(
        pack_kernel,
        "pack",
        [vmem] * len(pieces),
        [floats((2 * assets + 1) * own_slabs, lanes)],
    )(*pieces)
    places = lax.broadcasted_iota(jnp.int32, (1, assets), 1)
    last = jnp.where(places == 0, date_index.astype(jnp.float32), jnp.where(places == 1, strike, 0.0))
    table = jnp.concatenate([vol_table, last], axis=0)
    columns, payoff = local_call(
        side_kernel, "side", [vmem, vmem], [floats(2, assets, lanes), floats(own_slabs, lanes)]
    )(table, packed)

    slabs = own_slabs
    mask = blk_size // 2
    while mask > 2:
        received = across(packed, mask)
        cuts = (0, assets * slabs, 2 * assets * slabs, (2 * assets + 1) * slabs)
        packed = jnp.concatenate(
            [part[a:b] for a, b in zip(cuts, cuts[1:]) for part in (packed, received)], axis=0
        )
        if slabs == own_slabs:
            packed, columns, payoff = lax.optimization_barrier((packed, columns, payoff))
        slabs *= 2
        mask //= 2
    sources = assets * slabs
    nodes = slabs * lanes
    far = across(packed, 2)
    other = across(packed[sources:], 1)
    left, right, base = local_call(
        functools.partial(column_kernel, sources),
        "column",
        [vmem, vmem],
        [halves(nodes, depth), halves(depth, nodes), floats(slabs, lanes)],
        nodes * nodes,
    )(columns, packed)
    other_right, other_base = local_call(
        column_other_kernel,
        "column_other",
        [vmem] * 3,
        [halves(depth, nodes), floats(slabs, lanes)],
        nodes * nodes,
    )(columns, other, left)
    far_other = across(far[sources:], 1)
    far_left, far_right, density = local_call(
        functools.partial(far_kernel, sources),
        "far",
        [vmem] * 5,
        [halves(nodes, depth), halves(depth, nodes), floats(2 * slabs, lanes)],
        3 * nodes * nodes,
    )(columns, far, left, right, base)
    far_other_right, other_density = local_call(
        far_other_kernel,
        "far_other",
        [vmem] * 6,
        [halves(depth, nodes), floats(2 * slabs, lanes)],
        3 * nodes * nodes,
    )(columns, far_other, left, far_left, other_right, other_base)
    density = jnp.concatenate([density, other_density], axis=0)
    received = across(density, 1)
    (matrix,) = local_call(
        matrix_kernel, "matrix", [vmem] * 5, [floats(count, 4 * nodes)], 4 * count * nodes
    )(left[:count], right, far_right, other_right, far_other_right)
    continuation, node_value = local_call(
        functools.partial(weight_kernel, 2 * sources),
        "weights",
        [vmem] * 8,
        [floats(own_slabs, lanes)] * 2,
        scratch_shapes=[pltpu.VMEM((2, 4 * slabs, lanes), jnp.float32)],
    )(matrix, density, received, packed, far, other, far_other, payoff)
    return continuation.reshape(count), node_value.reshape(count)


def solution(mesh):
    blk_size = mesh.shape["blk"]
    placed = (
        P(None, ("groups", "blk")),
        P(None, ("groups", "blk")),
        P(("groups", "blk")),
        P(),
        P(),
        P(),
    )
    doubled = blk_size in (16, 32)
    return jax.shard_map(
        functools.partial(doubled_body, blk_size) if doubled else gathered_body,
        mesh=mesh,
        in_specs=placed,
        out_specs=(P(("groups", "blk")), P(("groups", "blk"))),
        check_vma=False,
    )
```

```python
import functools
import math

import jax
import jax.numpy as jnp
from jax import lax
from jax.experimental import pallas as pl
from jax.experimental.pallas import tpu as pltpu
from jax.sharding import PartitionSpec as P


rate_year = 0.05
step_years = 0.1
log2_e = math.log2(math.e)
lanes = 128
lane_tile = 512
row_tile = 256
depth = 128
vmem_grant = 16 * 1024 * 1024


def scaled_states(current_states, next_states, vol_table, date_index):
    date_count = vol_table.shape[0]
    picked = (jnp.arange(date_count, dtype=jnp.int32) == date_index[0]).astype(jnp.float32)
    vol_row = jnp.sum(vol_table * picked[:, None], axis=0)
    spread = vol_row * math.sqrt(step_years)
    drift_term = (rate_year - 0.5 * vol_row * vol_row) * step_years
    anchor = (current_states + drift_term[:, None]) / spread[:, None]
    target = next_states / spread[:, None]
    anchor_half = 0.5 * jnp.sum(anchor * anchor, axis=0, keepdims=True)
    target_half = 0.5 * jnp.sum(target * target, axis=0, keepdims=True)
    return (anchor, anchor_half, target, target_half)


def kernel_block(source_states, source_norms, sink_states, sink_norms):
    inner_term = lax.dot_general(
        source_states,
        sink_states,
        (((0,), (0,)), ((), ())),
        precision=lax.Precision.HIGHEST,
        preferred_element_type=jnp.float32,
    )
    return jnp.exp(inner_term - source_norms.reshape(-1, 1) - sink_norms)


def block_rows(row_count):
    if row_count <= 4096:
        return row_count
    return math.gcd(row_count, 4096)


def finish(current_states, totals, strike):
    continuation = math.exp(-rate_year * step_years) * totals[0] / totals[1]
    payoff = jnp.maximum(jnp.max(jnp.exp(current_states), axis=0) - strike[0], 0.0)
    return (continuation, jnp.maximum(payoff, continuation))


def gathered_body(current_states, next_states, next_values, vol_table, date_index, strike):
    anchor, anchor_half, target, target_half = scaled_states(
        current_states, next_states, vol_table, date_index
    )
    local_count = anchor.shape[1]
    pieces = (
        lax.all_gather(anchor, "blk", axis=1, tiled=True),
        lax.all_gather(anchor_half, "blk", axis=1, tiled=True),
    )
    row_count = pieces[0].shape[1]
    block_size = block_rows(row_count)

    def density_block(number, inner_sum):
        source_part = lax.dynamic_slice_in_dim(pieces[0], number * block_size, block_size, 1)
        norm_part = lax.dynamic_slice_in_dim(pieces[1], number * block_size, block_size, 1)
        return inner_sum + jnp.sum(
            kernel_block(source_part, norm_part, target, target_half), axis=0
        )

    density = lax.fori_loop(
        0, row_count // block_size, density_block, jnp.zeros((local_count,), jnp.float32)
    )
    extras = jnp.concatenate(
        [target_half, (next_values / density)[None, :], (1.0 / density)[None, :]], axis=0
    )
    add_pieces = (
        lax.all_gather(target, "blk", axis=1, tiled=True),
        lax.all_gather(extras, "blk", axis=1, tiled=True),
    )

    def weighted_block(number, inner_sum):
        sink_part = lax.dynamic_slice_in_dim(add_pieces[0], number * block_size, block_size, 1)
        extra_part = lax.dynamic_slice_in_dim(add_pieces[1], number * block_size, block_size, 1)
        weights = kernel_block(sink_part, extra_part[0:1], anchor, anchor_half)
        return inner_sum + jnp.dot(
            extra_part[1:3],
            weights,
            precision=lax.Precision.HIGHEST,
            preferred_element_type=jnp.float32,
        )

    totals = lax.fori_loop(
        0, row_count // block_size, weighted_block, jnp.zeros((2, local_count), jnp.float32)
    )
    return finish(current_states, totals, strike)


def in_three(x):
    first = x.astype(jnp.bfloat16)
    rest = x - first.astype(jnp.float32)
    second = rest.astype(jnp.bfloat16)
    third = (rest - second.astype(jnp.float32)).astype(jnp.bfloat16)
    return first, second, third


def with_norm(pieces, norm, shift):
    rows = lax.broadcasted_iota(jnp.int32, (16, norm.shape[1]), 0)
    tile = jnp.where((rows >= 3 - shift) & (rows < 6 - shift), 1.0, 0.0)
    for k, part in enumerate(in_three(norm)):
        tile = jnp.where(rows == k + shift, part.astype(jnp.float32), tile)
    stacked = list(pieces) + [tile.astype(jnp.bfloat16)]
    height = sum(piece.shape[0] for piece in stacked)
    stacked.append(jnp.zeros((depth - height, norm.shape[1]), jnp.bfloat16))
    return jnp.concatenate(stacked, axis=0)


def source_operand(states, inverse, drift_term):
    anchor = (states + drift_term) * inverse
    half = (0.5 * log2_e) * jnp.sum(anchor * anchor, axis=0, keepdims=True)
    a1, a2, a3 = in_three(anchor * log2_e)
    return with_norm((a1, a1, a2, a1, a2, a3), -half, 0).T


def sink_operand(states, inverse):
    target = states * inverse
    half = (0.5 * log2_e) * jnp.sum(target * target, axis=0, keepdims=True)
    t1, t2, t3 = in_three(target)
    return with_norm((t1, t2, t1, t3, t2, t1), -half, 3)


def build_sources(states_refs, columns_ref, left_ref):
    inverse, drift_term = columns_ref[0], columns_ref[1]
    assets = inverse.shape[0]
    slabs = left_ref.shape[0] // lanes // len(states_refs)
    for slab in range(left_ref.shape[0] // lanes):
        row = slab % slabs * assets
        states = states_refs[slab // slabs][row : row + assets, :]
        left_ref[slab * lanes : (slab + 1) * lanes, :] = source_operand(states, inverse, drift_term)


def build_sinks(states_refs, start, columns_ref, right_ref):
    inverse = columns_ref[0]
    assets = inverse.shape[0]
    slabs = right_ref.shape[1] // lanes // len(states_refs)
    for slab in range(right_ref.shape[1] // lanes):
        row = start + slab % slabs * assets
        states = states_refs[slab // slabs][row : row + assets, :]
        right_ref[:, slab * lanes : (slab + 1) * lanes] = sink_operand(states, inverse)


def add_density(left_refs, right_ref, density_ref, first_row, base_ref):
    width = math.gcd(right_ref.shape[1], lane_tile)
    for number in range(right_ref.shape[1] // width):
        right = right_ref[:, number * width : (number + 1) * width]
        total = jnp.zeros((8, width), jnp.float32)
        for left_ref in left_refs:
            height = math.gcd(left_ref.shape[0], row_tile)
            for k in range(left_ref.shape[0] // height):
                exponent = jnp.dot(
                    left_ref[k * height : (k + 1) * height, :],
                    right,
                    preferred_element_type=jnp.float32,
                )
                total += jnp.sum(jnp.exp2(exponent).reshape(height // 8, 8, width), axis=0)
        sums = jnp.sum(total, axis=0, keepdims=True)
        for slab in range(width // lanes):
            row = number * (width // lanes) + slab
            value = sums[:, slab * lanes : (slab + 1) * lanes]
            if base_ref is not None:
                value += base_ref[row : row + 1, :]
            density_ref[first_row + row : first_row + row + 1, :] = value


def pack_kernel(*refs):
    row = 0
    for ref in refs[:-1]:
        height = min(ref.shape[0], refs[-1].shape[0] - row)
        refs[-1][row : row + height, :] = ref[0:height, :]
        row += height


def columns_kernel(table_ref, packed_ref, columns_ref):
    dates, assets = table_ref.shape[0] - 1, table_ref.shape[1]
    index = table_ref[dates : dates + 1, 0:1]
    rows = lax.broadcasted_iota(jnp.int32, (dates, assets), 0).astype(jnp.float32)
    vol_row = jnp.sum(
        jnp.where(rows == index, table_ref[0:dates, :], 0.0), axis=0, keepdims=True
    )
    square = (assets, assets)
    diagonal = lax.broadcasted_iota(jnp.int32, square, 0) == lax.broadcasted_iota(
        jnp.int32, square, 1
    )
    vol = jnp.sum(
        jnp.where(diagonal, jnp.broadcast_to(vol_row, square), 0.0), axis=1, keepdims=True
    )
    vol = jnp.broadcast_to(vol, (assets, lanes))
    columns_ref[0] = 1.0 / (vol * math.sqrt(step_years))
    columns_ref[1] = (rate_year - 0.5 * vol * vol) * step_years


def payoff_kernel(table_ref, packed_ref, payoff_ref):
    assets = table_ref.shape[1]
    strike = table_ref[table_ref.shape[0] - 1 :, 1:2]
    for slab in range(payoff_ref.shape[0]):
        prices = jnp.exp(packed_ref[slab * assets : (slab + 1) * assets, :])
        best = jnp.max(prices, axis=0, keepdims=True)
        payoff_ref[slab : slab + 1, :] = jnp.maximum(best - strike, 0.0)


def near_kernel(sources, columns_ref, first_ref, second_ref, left_ref, right_ref, density_ref):
    build_sources((first_ref, second_ref), columns_ref, left_ref)
    build_sinks((first_ref, second_ref), sources, columns_ref, right_ref)
    add_density((left_ref,), right_ref, density_ref, 0, None)


def near_other_kernel(columns_ref, other_ref, left_ref, right_ref, density_ref):
    build_sinks((other_ref,), 0, columns_ref, right_ref)
    add_density((left_ref,), right_ref, density_ref, 0, None)


def far_kernel(
    sources,
    columns_ref,
    first_ref,
    second_ref,
    left_ref,
    right_ref,
    base_ref,
    far_left_ref,
    far_right_ref,
    density_ref,
):
    build_sources((first_ref, second_ref), columns_ref, far_left_ref)
    build_sinks((first_ref, second_ref), sources, columns_ref, far_right_ref)
    add_density((far_left_ref,), right_ref, density_ref, 0, base_ref)
    add_density((left_ref, far_left_ref), far_right_ref, density_ref, base_ref.shape[0], None)


def far_other_kernel(
    columns_ref,
    other_ref,
    left_ref,
    far_left_ref,
    right_ref,
    base_ref,
    far_right_ref,
    density_ref,
):
    build_sinks((other_ref,), 0, columns_ref, far_right_ref)
    add_density((far_left_ref,), right_ref, density_ref, 0, base_ref)
    add_density((left_ref, far_left_ref), far_right_ref, density_ref, base_ref.shape[0], None)


def matrix_kernel(left_ref, *refs):
    matrix_ref = refs[-1]
    place = 0
    for right_ref in refs[:-1]:
        width = math.gcd(right_ref.shape[1], lane_tile)
        for number in range(right_ref.shape[1] // width):
            matrix_ref[:, place : place + width] = jnp.exp2(
                jnp.dot(
                    left_ref[...],
                    right_ref[:, number * width : (number + 1) * width],
                    preferred_element_type=jnp.float32,
                )
            )
            place += width


def weight_kernel(matrix_ref, density_ref, received_ref, *refs):
    *values_refs, payoff_ref, continuation_ref, node_ref, ratio_ref = refs
    slabs = density_ref.shape[0]
    half = slabs // 2
    inverse = 1.0 / jnp.concatenate(
        [
            density_ref[:half, :] + received_ref[half:, :],
            density_ref[half:, :] + received_ref[:half, :],
        ],
        axis=0,
    )
    ratio_ref[1] = inverse
    assets_twice = 2 * (values_refs[-1].shape[0] // (slabs // 4) - 1)
    row = 0
    for k, values_ref in enumerate(values_refs):
        rows_per_slab = assets_twice + 1 if k < 4 else assets_twice // 2 + 1
        count = values_ref.shape[0] // rows_per_slab
        values = values_ref[values_ref.shape[0] - count :, :]
        ratio_ref[0, row : row + count, :] = values * inverse[row : row + count]
        row += count
    count = matrix_ref.shape[0]
    height = math.gcd(count, 64)
    sums = []
    for k in range(count // height):
        weighted = jnp.zeros((height, lanes), jnp.float32)
        mass = jnp.zeros((height, lanes), jnp.float32)
        for slab in range(slabs):
            piece = matrix_ref[k * height : (k + 1) * height, slab * lanes : (slab + 1) * lanes]
            weighted += piece * ratio_ref[0, slab : slab + 1, :]
            mass += piece * ratio_ref[1, slab : slab + 1, :]
        sums.append((weighted, mass))
    per_slab = lanes // height
    for slab in range(count // lanes):
        group = sums[slab * per_slab : (slab + 1) * per_slab]
        weighted, mass = (
            jnp.sum(jnp.concatenate([pair[k] for pair in group], axis=0).T, axis=0, keepdims=True)
            for k in range(2)
        )
        continuation = math.exp(-rate_year * step_years) * weighted / mass
        continuation_ref[slab : slab + 1, :] = continuation
        node_ref[slab : slab + 1, :] = jnp.maximum(payoff_ref[slab : slab + 1, :], continuation)


vmem = pl.BlockSpec(memory_space=pltpu.VMEM)


def local_call(kernel, in_specs, out_shapes, matmul_pairs=0, scratch_shapes=()):
    cost = pl.CostEstimate(
        flops=2 * depth * matmul_pairs, transcendentals=matmul_pairs, bytes_accessed=0
    )
    return pl.pallas_call(
        kernel,
        out_shape=out_shapes,
        in_specs=in_specs,
        out_specs=[vmem] * len(out_shapes),
        scratch_shapes=scratch_shapes,
        cost_estimate=cost,
        compiler_params=pltpu.CompilerParams(vmem_limit_bytes=vmem_grant),
    )


def doubled_body(blk_size, current_states, next_states, next_values, vol_table, date_index, strike):
    assets, count = current_states.shape
    own_slabs = count // lanes

    def across(array, mask):
        return lax.ppermute(array, "blk", [(i, i ^ mask) for i in range(blk_size)])

    def floats(*shape):
        return jax.ShapeDtypeStruct(shape, jnp.float32)

    def halves(*shape):
        return jax.ShapeDtypeStruct(shape, jnp.bfloat16)

    pieces = [
        part[:, slab * lanes : (slab + 1) * lanes]
        for part in (current_states, next_states)
        for slab in range(own_slabs)
    ]
    rows = lax.pad(
        next_values.reshape(own_slabs, lanes), jnp.float32(0), ((0, assets - own_slabs, 0), (0, 0, 0))
    )
    tile_rows = lax.broadcasted_iota(jnp.int32, rows.shape, 0)
    pieces.append(jnp.where(tile_rows < own_slabs, rows, pieces[0]))
    (packed,) = local_call(
        pack_kernel, [vmem] * len(pieces), [floats((2 * assets + 1) * own_slabs, lanes)]
    )(*pieces)
    places = lax.broadcasted_iota(jnp.int32, (1, assets), 1)
    last = jnp.where(places == 0, date_index.astype(jnp.float32), jnp.where(places == 1, strike, 0.0))
    table = jnp.concatenate([vol_table, last], axis=0)
    (columns,) = local_call(columns_kernel, [vmem, vmem], [floats(2, assets, lanes)])(table, packed)

    slabs = own_slabs
    mask = blk_size // 2
    while mask > 4:
        received = across(packed, mask)
        cuts = (0, assets * slabs, 2 * assets * slabs, (2 * assets + 1) * slabs)
        packed = jnp.concatenate(
            [part[a:b] for a, b in zip(cuts, cuts[1:]) for part in (packed, received)], axis=0
        )
        if slabs == own_slabs:
            packed, columns = lax.optimization_barrier((packed, columns))
        slabs *= 2
        mask //= 2
    sources = assets * slabs
    near = across(packed, 2)
    far_first = across(packed, 6)
    far_second = across(packed, 4)

    (payoff,) = local_call(payoff_kernel, [vmem, vmem], [floats(own_slabs, lanes)])(table, packed)

    def sinks(first, second):
        targets, values = slice(sources, 2 * sources), slice(2 * sources, None)
        return jnp.concatenate([first[targets], second[targets], first[values], second[values]])

    slabs *= 2
    nodes = slabs * lanes
    near_other = across(sinks(packed, near), 1)
    left, right, base = local_call(
        functools.partial(near_kernel, sources),
        [vmem] * 3,
        [halves(nodes, depth), halves(depth, nodes), floats(slabs, lanes)],
        nodes * nodes,
    )(columns, packed, near)
    other_right, other_base = local_call(
        near_other_kernel, [vmem] * 3, [halves(depth, nodes), floats(slabs, lanes)], nodes * nodes
    )(columns, near_other, left)
    far_other = across(sinks(far_first, far_second), 1)
    far_left, far_right, density = local_call(
        functools.partial(far_kernel, sources),
        [vmem] * 6,
        [halves(nodes, depth), halves(depth, nodes), floats(2 * slabs, lanes)],
        3 * nodes * nodes,
    )(columns, far_first, far_second, left, right, base)
    far_other_right, other_density = local_call(
        far_other_kernel,
        [vmem] * 6,
        [halves(depth, nodes), floats(2 * slabs, lanes)],
        3 * nodes * nodes,
    )(columns, far_other, left, far_left, other_right, other_base)
    density = jnp.concatenate([density, other_density], axis=0)
    received = across(density, 1)
    (matrix,) = local_call(
        matrix_kernel, [vmem] * 5, [floats(count, 4 * nodes)], 4 * count * nodes
    )(left[:count], right, far_right, other_right, far_other_right)
    continuation, node_value = local_call(
        weight_kernel,
        [vmem] * 10,
        [floats(own_slabs, lanes)] * 2,
        scratch_shapes=[pltpu.VMEM((2, 4 * slabs, lanes), jnp.float32)],
    )(
        matrix,
        density,
        received,
        packed,
        near,
        far_first,
        far_second,
        near_other,
        far_other,
        payoff,
    )
    return continuation.reshape(count), node_value.reshape(count)


def solution(mesh):
    blk_size = mesh.shape["blk"]
    placed = (
        P(None, ("groups", "blk")),
        P(None, ("groups", "blk")),
        P(("groups", "blk")),
        P(),
        P(),
        P(),
    )
    doubled = blk_size in (16, 32)
    return jax.shard_map(
        functools.partial(doubled_body, blk_size) if doubled else gathered_body,
        mesh=mesh,
        in_specs=placed,
        out_specs=(P(("groups", "blk")), P(("groups", "blk"))),
        check_vma=False,
    )
```

```python
import functools
import math

import jax
import jax.numpy as jnp
from jax import lax
from jax.experimental import pallas as pl
from jax.experimental.pallas import tpu as pltpu
from jax.sharding import PartitionSpec as P


rate_year = 0.05
step_years = 0.1
log2_e = math.log2(math.e)
lanes = 128
lane_tile = 512
row_tile = 1024
depth = 128
vmem_grant = 16 * 1024 * 1024 + 4096


def scaled_states(current_states, next_states, vol_table, date_index):
    date_count = vol_table.shape[0]
    picked = (jnp.arange(date_count, dtype=jnp.int32) == date_index[0]).astype(jnp.float32)
    vol_row = jnp.sum(vol_table * picked[:, None], axis=0)
    spread = vol_row * math.sqrt(step_years)
    drift_term = (rate_year - 0.5 * vol_row * vol_row) * step_years
    anchor = (current_states + drift_term[:, None]) / spread[:, None]
    target = next_states / spread[:, None]
    anchor_half = 0.5 * jnp.sum(anchor * anchor, axis=0, keepdims=True)
    target_half = 0.5 * jnp.sum(target * target, axis=0, keepdims=True)
    return (anchor, anchor_half, target, target_half)


def kernel_block(source_states, source_norms, sink_states, sink_norms):
    inner_term = lax.dot_general(
        source_states,
        sink_states,
        (((0,), (0,)), ((), ())),
        precision=lax.Precision.HIGHEST,
        preferred_element_type=jnp.float32,
    )
    return jnp.exp(inner_term - source_norms.reshape(-1, 1) - sink_norms)


def block_rows(row_count):
    if row_count <= 4096:
        return row_count
    return math.gcd(row_count, 4096)


def finish(current_states, totals, strike):
    continuation = math.exp(-rate_year * step_years) * totals[0] / totals[1]
    payoff = jnp.maximum(jnp.max(jnp.exp(current_states), axis=0) - strike[0], 0.0)
    return (continuation, jnp.maximum(payoff, continuation))


def gathered_body(current_states, next_states, next_values, vol_table, date_index, strike):
    anchor, anchor_half, target, target_half = scaled_states(
        current_states, next_states, vol_table, date_index
    )
    local_count = anchor.shape[1]
    pieces = (
        lax.all_gather(anchor, "blk", axis=1, tiled=True),
        lax.all_gather(anchor_half, "blk", axis=1, tiled=True),
    )
    row_count = pieces[0].shape[1]
    block_size = block_rows(row_count)

    def density_block(number, inner_sum):
        source_part = lax.dynamic_slice_in_dim(pieces[0], number * block_size, block_size, 1)
        norm_part = lax.dynamic_slice_in_dim(pieces[1], number * block_size, block_size, 1)
        return inner_sum + jnp.sum(
            kernel_block(source_part, norm_part, target, target_half), axis=0
        )

    density = lax.fori_loop(
        0, row_count // block_size, density_block, jnp.zeros((local_count,), jnp.float32)
    )
    extras = jnp.concatenate(
        [target_half, (next_values / density)[None, :], (1.0 / density)[None, :]], axis=0
    )
    add_pieces = (
        lax.all_gather(target, "blk", axis=1, tiled=True),
        lax.all_gather(extras, "blk", axis=1, tiled=True),
    )

    def weighted_block(number, inner_sum):
        sink_part = lax.dynamic_slice_in_dim(add_pieces[0], number * block_size, block_size, 1)
        extra_part = lax.dynamic_slice_in_dim(add_pieces[1], number * block_size, block_size, 1)
        weights = kernel_block(sink_part, extra_part[0:1], anchor, anchor_half)
        return inner_sum + jnp.dot(
            extra_part[1:3],
            weights,
            precision=lax.Precision.HIGHEST,
            preferred_element_type=jnp.float32,
        )

    totals = lax.fori_loop(
        0, row_count // block_size, weighted_block, jnp.zeros((2, local_count), jnp.float32)
    )
    return finish(current_states, totals, strike)


def in_three(x):
    first = x.astype(jnp.bfloat16)
    rest = x - first.astype(jnp.float32)
    second = rest.astype(jnp.bfloat16)
    third = (rest - second.astype(jnp.float32)).astype(jnp.bfloat16)
    return first, second, third


def with_norm(pieces, norm, shift):
    rows = lax.broadcasted_iota(jnp.int32, (16, norm.shape[1]), 0)
    tile = jnp.where((rows >= 3 - shift) & (rows < 6 - shift), 1.0, 0.0)
    for k, part in enumerate(in_three(norm)):
        tile = jnp.where(rows == k + shift, part.astype(jnp.float32), tile)
    stacked = list(pieces) + [tile.astype(jnp.bfloat16)]
    height = sum(piece.shape[0] for piece in stacked)
    stacked.append(jnp.zeros((depth - height, norm.shape[1]), jnp.bfloat16))
    return jnp.concatenate(stacked, axis=0)


def source_operand(states, inverse, drift_term):
    anchor = (states + drift_term) * inverse
    half = (0.5 * log2_e) * jnp.sum(anchor * anchor, axis=0, keepdims=True)
    a1, a2, a3 = in_three(anchor * log2_e)
    return with_norm((a1, a1, a2, a1, a2, a3), -half, 0).T


def sink_operand(states, inverse):
    target = states * inverse
    half = (0.5 * log2_e) * jnp.sum(target * target, axis=0, keepdims=True)
    t1, t2, t3 = in_three(target)
    return with_norm((t1, t2, t1, t3, t2, t1), -half, 3)


def build_sources(states_refs, columns_ref, left_ref):
    inverse, drift_term = columns_ref[0], columns_ref[1]
    assets = inverse.shape[0]
    slabs = left_ref.shape[0] // lanes // len(states_refs)
    for slab in range(left_ref.shape[0] // lanes):
        row = slab % slabs * assets
        states = states_refs[slab // slabs][row : row + assets, :]
        left_ref[slab * lanes : (slab + 1) * lanes, :] = source_operand(states, inverse, drift_term)


def build_sinks(states_refs, start, columns_ref, right_ref):
    inverse = columns_ref[0]
    assets = inverse.shape[0]
    slabs = right_ref.shape[1] // lanes // len(states_refs)
    for slab in range(right_ref.shape[1] // lanes):
        row = start + slab % slabs * assets
        states = states_refs[slab // slabs][row : row + assets, :]
        right_ref[:, slab * lanes : (slab + 1) * lanes] = sink_operand(states, inverse)


def add_density(left_refs, right_ref, density_ref, first_row, base_ref=None, base_row=0):
    width = math.gcd(right_ref.shape[1], lane_tile)
    for number in range(right_ref.shape[1] // width):
        right = right_ref[:, number * width : (number + 1) * width]
        total = jnp.zeros((8, width), jnp.float32)
        for left_ref in left_refs:
            height = math.gcd(left_ref.shape[0], row_tile)
            for k in range(left_ref.shape[0] // height):
                exponent = jnp.dot(
                    left_ref[k * height : (k + 1) * height, :],
                    right,
                    preferred_element_type=jnp.float32,
                )
                total += jnp.sum(jnp.exp2(exponent).reshape(height // 8, 8, width), axis=0)
        sums = jnp.sum(total, axis=0, keepdims=True)
        for slab in range(width // lanes):
            row = number * (width // lanes) + slab
            value = sums[:, slab * lanes : (slab + 1) * lanes]
            if base_ref is not None:
                value += base_ref[base_row + row : base_row + row + 1, :]
            density_ref[first_row + row : first_row + row + 1, :] = value


def pack_kernel(*refs):
    row = 0
    for ref in refs[:-1]:
        height = min(ref.shape[0], refs[-1].shape[0] - row)
        refs[-1][row : row + height, :] = ref[0:height, :]
        row += height


def columns_kernel(table_ref, packed_ref, columns_ref):
    dates, assets = table_ref.shape[0] - 1, table_ref.shape[1]
    index = table_ref[dates : dates + 1, 0:1]
    rows = lax.broadcasted_iota(jnp.int32, (dates, assets), 0).astype(jnp.float32)
    vol_row = jnp.sum(
        jnp.where(rows == index, table_ref[0:dates, :], 0.0), axis=0, keepdims=True
    )
    square = (assets, assets)
    diagonal = lax.broadcasted_iota(jnp.int32, square, 0) == lax.broadcasted_iota(
        jnp.int32, square, 1
    )
    vol = jnp.sum(
        jnp.where(diagonal, jnp.broadcast_to(vol_row, square), 0.0), axis=1, keepdims=True
    )
    vol = jnp.broadcast_to(vol, (assets, lanes))
    columns_ref[0] = 1.0 / (vol * math.sqrt(step_years))
    columns_ref[1] = (rate_year - 0.5 * vol * vol) * step_years


def payoff_kernel(table_ref, packed_ref, payoff_ref):
    assets = table_ref.shape[1]
    strike = table_ref[table_ref.shape[0] - 1 :, 1:2]
    for slab in range(payoff_ref.shape[0]):
        prices = jnp.exp(packed_ref[slab * assets : (slab + 1) * assets, :])
        best = jnp.max(prices, axis=0, keepdims=True)
        payoff_ref[slab : slab + 1, :] = jnp.maximum(best - strike, 0.0)


def near_kernel(sources, columns_ref, first_ref, second_ref, left_ref, right_ref, density_ref):
    build_sources((first_ref, second_ref), columns_ref, left_ref)
    build_sinks((first_ref, second_ref), sources, columns_ref, right_ref)
    add_density((left_ref,), right_ref, density_ref, 0)


def near_other_kernel(columns_ref, other_ref, left_ref, right_ref, density_ref):
    build_sinks((other_ref,), 0, columns_ref, right_ref)
    add_density((left_ref,), right_ref, density_ref, 0)


def mid_kernel(sources, columns_ref, mid_ref, near_left, near_right, base, left, right, density):
    build_sinks((mid_ref,), sources, columns_ref, right)
    build_sources((mid_ref,), columns_ref, left)
    add_density((near_left, left), right, density, base.shape[0])
    add_density((left,), near_right, density, 0, base)


def far_kernel(
    sources,
    columns_ref,
    far_ref,
    near_left,
    mid_left,
    near_right,
    mid_right,
    base,
    left,
    right,
    density,
):
    near_slabs = near_right.shape[1] // lanes
    build_sinks((far_ref,), sources, columns_ref, right)
    build_sources((far_ref,), columns_ref, left)
    add_density((near_left, mid_left, left), right, density, base.shape[0])
    add_density((left,), near_right, density, 0, base)
    add_density((left,), mid_right, density, near_slabs, base, near_slabs)


def far_other_kernel(
    columns_ref,
    other_ref,
    near_left,
    mid_left,
    far_left,
    near_right,
    base,
    right,
    density,
):
    add_density((mid_left, far_left), near_right, density, 0, base)
    build_sinks((other_ref,), 0, columns_ref, right)
    add_density((near_left, mid_left, far_left), right, density, base.shape[0])


def matrix_kernel(left_ref, *refs):
    matrix_ref = refs[-1]
    place = 0
    for right_ref in refs[:-1]:
        width = math.gcd(right_ref.shape[1], lane_tile)
        for number in range(right_ref.shape[1] // width):
            matrix_ref[:, place : place + width] = jnp.exp2(
                jnp.dot(
                    left_ref[...],
                    right_ref[:, number * width : (number + 1) * width],
                    preferred_element_type=jnp.float32,
                )
            )
            place += width


def weight_kernel(assets, matrix_ref, density_ref, received_ref, *refs):
    *values_refs, payoff_ref, continuation_ref, node_ref, ratio_ref = refs
    slabs = density_ref.shape[0]
    half = slabs // 2
    inverse = 1.0 / jnp.concatenate(
        [
            density_ref[:half, :] + received_ref[half:, :],
            density_ref[half:, :] + received_ref[:half, :],
        ],
        axis=0,
    )
    ratio_ref[1] = inverse
    row = 0
    for k, values_ref in enumerate(values_refs):
        rows_per_slab = 2 * assets + 1 if k < 4 else assets + 1
        count = values_ref.shape[0] // rows_per_slab
        values = values_ref[values_ref.shape[0] - count :, :]
        ratio_ref[0, row : row + count, :] = values * inverse[row : row + count]
        row += count
    count = matrix_ref.shape[0]
    height = math.gcd(count, 64)
    sums = []
    for k in range(count // height):
        weighted = jnp.zeros((height, lanes), jnp.float32)
        mass = jnp.zeros((height, lanes), jnp.float32)
        for slab in range(slabs):
            piece = matrix_ref[k * height : (k + 1) * height, slab * lanes : (slab + 1) * lanes]
            weighted += piece * ratio_ref[0, slab : slab + 1, :]
            mass += piece * ratio_ref[1, slab : slab + 1, :]
        sums.append((weighted, mass))
    per_slab = lanes // height
    for slab in range(count // lanes):
        group = sums[slab * per_slab : (slab + 1) * per_slab]
        weighted, mass = (
            jnp.sum(jnp.concatenate([pair[k] for pair in group], axis=0).T, axis=0, keepdims=True)
            for k in range(2)
        )
        continuation = math.exp(-rate_year * step_years) * weighted / mass
        continuation_ref[slab : slab + 1, :] = continuation
        node_ref[slab : slab + 1, :] = jnp.maximum(payoff_ref[slab : slab + 1, :], continuation)


vmem = pl.BlockSpec(memory_space=pltpu.VMEM)


def local_call(kernel, in_specs, out_shapes, matmul_pairs=0, scratch_shapes=()):
    cost = pl.CostEstimate(
        flops=2 * depth * matmul_pairs, transcendentals=matmul_pairs, bytes_accessed=0
    )
    return pl.pallas_call(
        kernel,
        out_shape=out_shapes,
        in_specs=in_specs,
        out_specs=[vmem] * len(out_shapes),
        scratch_shapes=scratch_shapes,
        cost_estimate=cost,
        compiler_params=pltpu.CompilerParams(vmem_limit_bytes=vmem_grant),
    )


def doubled_body(blk_size, current_states, next_states, next_values, vol_table, date_index, strike):
    assets, count = current_states.shape
    own_slabs = count // lanes

    def across(array, mask):
        return lax.ppermute(array, "blk", [(i, i ^ mask) for i in range(blk_size)])

    def floats(*shape):
        return jax.ShapeDtypeStruct(shape, jnp.float32)

    def halves(*shape):
        return jax.ShapeDtypeStruct(shape, jnp.bfloat16)

    pieces = [
        part[:, slab * lanes : (slab + 1) * lanes]
        for part in (current_states, next_states)
        for slab in range(own_slabs)
    ]
    rows = lax.pad(
        next_values.reshape(own_slabs, lanes), jnp.float32(0), ((0, assets - own_slabs, 0), (0, 0, 0))
    )
    tile_rows = lax.broadcasted_iota(jnp.int32, rows.shape, 0)
    pieces.append(jnp.where(tile_rows < own_slabs, rows, pieces[0]))
    (packed,) = local_call(
        pack_kernel, [vmem] * len(pieces), [floats((2 * assets + 1) * own_slabs, lanes)]
    )(*pieces)
    places = lax.broadcasted_iota(jnp.int32, (1, assets), 1)
    last = jnp.where(places == 0, date_index.astype(jnp.float32), jnp.where(places == 1, strike, 0.0))
    table = jnp.concatenate([vol_table, last], axis=0)
    (columns,) = local_call(columns_kernel, [vmem, vmem], [floats(2, assets, lanes)])(table, packed)

    slabs = own_slabs
    mask = blk_size // 2
    while mask > 4:
        received = across(packed, mask)
        cuts = (0, assets * slabs, 2 * assets * slabs, (2 * assets + 1) * slabs)
        packed = jnp.concatenate(
            [part[a:b] for a, b in zip(cuts, cuts[1:]) for part in (packed, received)], axis=0
        )
        if slabs == own_slabs:
            packed, columns = lax.optimization_barrier((packed, columns))
        slabs *= 2
        mask //= 2
    sources = assets * slabs
    near = across(packed, 4)
    mid = across(packed, 6)
    far = across(packed, 2)
    (payoff,) = local_call(payoff_kernel, [vmem, vmem], [floats(own_slabs, lanes)])(table, packed)
    nodes = slabs * lanes
    targets, values = slice(sources, 2 * sources), slice(2 * sources, None)

    def sinks(first, second):
        return jnp.concatenate([first[targets], second[targets], first[values], second[values]])

    near_other = across(sinks(packed, near), 1)
    left, right, base = local_call(
        functools.partial(near_kernel, sources),
        [vmem] * 3,
        [halves(2 * nodes, depth), halves(depth, 2 * nodes), floats(2 * slabs, lanes)],
        4 * nodes * nodes,
    )(columns, packed, near)
    other_right, other_base = local_call(
        near_other_kernel,
        [vmem] * 3,
        [halves(depth, 2 * nodes), floats(2 * slabs, lanes)],
        4 * nodes * nodes,
    )(columns, near_other, left)
    mid_left, mid_right, mid_base = local_call(
        functools.partial(mid_kernel, sources),
        [vmem] * 5,
        [halves(nodes, depth), halves(depth, nodes), floats(3 * slabs, lanes)],
        5 * nodes * nodes,
    )(columns, mid, left, right, base)
    far_other = across(sinks(mid, far), 1)
    far_left, far_right, density = local_call(
        functools.partial(far_kernel, sources),
        [vmem] * 7,
        [halves(nodes, depth), halves(depth, nodes), floats(4 * slabs, lanes)],
        7 * nodes * nodes,
    )(columns, far, left, mid_left, right, mid_right, mid_base)
    far_other_right, other_density = local_call(
        far_other_kernel,
        [vmem] * 7,
        [halves(depth, 2 * nodes), floats(4 * slabs, lanes)],
        12 * nodes * nodes,
    )(columns, far_other, left, mid_left, far_left, other_right, other_base)
    density = jnp.concatenate([density, other_density], axis=0)
    received = across(density, 1)
    (matrix,) = local_call(
        matrix_kernel, [vmem] * 6, [floats(count, 8 * nodes)], 8 * count * nodes
    )(left[:count], right, mid_right, far_right, other_right, far_other_right)
    continuation, node_value = local_call(
        functools.partial(weight_kernel, assets),
        [vmem] * 10,
        [floats(own_slabs, lanes)] * 2,
        scratch_shapes=[pltpu.VMEM((2, 8 * slabs, lanes), jnp.float32)],
    )(
        matrix,
        density,
        received,
        packed,
        near,
        mid,
        far,
        near_other,
        far_other,
        payoff,
    )
    return continuation.reshape(count), node_value.reshape(count)


def solution(mesh):
    blk_size = mesh.shape["blk"]
    placed = (
        P(None, ("groups", "blk")),
        P(None, ("groups", "blk")),
        P(("groups", "blk")),
        P(),
        P(),
        P(),
    )
    doubled = blk_size in (16, 32)
    return jax.shard_map(
        functools.partial(doubled_body, blk_size) if doubled else gathered_body,
        mesh=mesh,
        in_specs=placed,
        out_specs=(P(("groups", "blk")), P(("groups", "blk"))),
        check_vma=False,
    )
```

```python
import functools
import math

import jax
import jax.numpy as jnp
from jax import lax
from jax.experimental import pallas as pl
from jax.experimental.pallas import tpu as pltpu
from jax.sharding import PartitionSpec as P


rate_year = 0.05
step_years = 0.1
log2_e = math.log2(math.e)
lanes = 128
lane_tile = 512
row_tile = 1024
depth = 128
vmem_grant = 16 * 1024 * 1024 + 4096


def scaled_states(current_states, next_states, vol_table, date_index):
    date_count = vol_table.shape[0]
    picked = (jnp.arange(date_count, dtype=jnp.int32) == date_index[0]).astype(jnp.float32)
    vol_row = jnp.sum(vol_table * picked[:, None], axis=0)
    spread = vol_row * math.sqrt(step_years)
    drift_term = (rate_year - 0.5 * vol_row * vol_row) * step_years
    anchor = (current_states + drift_term[:, None]) / spread[:, None]
    target = next_states / spread[:, None]
    anchor_half = 0.5 * jnp.sum(anchor * anchor, axis=0, keepdims=True)
    target_half = 0.5 * jnp.sum(target * target, axis=0, keepdims=True)
    return (anchor, anchor_half, target, target_half)


def kernel_block(source_states, source_norms, sink_states, sink_norms):
    inner_term = lax.dot_general(
        source_states,
        sink_states,
        (((0,), (0,)), ((), ())),
        precision=lax.Precision.HIGHEST,
        preferred_element_type=jnp.float32,
    )
    return jnp.exp(inner_term - source_norms.reshape(-1, 1) - sink_norms)


def block_rows(row_count):
    if row_count <= 4096:
        return row_count
    return math.gcd(row_count, 4096)


def finish(current_states, totals, strike):
    continuation = math.exp(-rate_year * step_years) * totals[0] / totals[1]
    payoff = jnp.maximum(jnp.max(jnp.exp(current_states), axis=0) - strike[0], 0.0)
    return (continuation, jnp.maximum(payoff, continuation))


def gathered_body(current_states, next_states, next_values, vol_table, date_index, strike):
    anchor, anchor_half, target, target_half = scaled_states(
        current_states, next_states, vol_table, date_index
    )
    local_count = anchor.shape[1]
    pieces = (
        lax.all_gather(anchor, "blk", axis=1, tiled=True),
        lax.all_gather(anchor_half, "blk", axis=1, tiled=True),
    )
    row_count = pieces[0].shape[1]
    block_size = block_rows(row_count)

    def density_block(number, inner_sum):
        source_part = lax.dynamic_slice_in_dim(pieces[0], number * block_size, block_size, 1)
        norm_part = lax.dynamic_slice_in_dim(pieces[1], number * block_size, block_size, 1)
        return inner_sum + jnp.sum(
            kernel_block(source_part, norm_part, target, target_half), axis=0
        )

    density = lax.fori_loop(
        0, row_count // block_size, density_block, jnp.zeros((local_count,), jnp.float32)
    )
    extras = jnp.concatenate(
        [target_half, (next_values / density)[None, :], (1.0 / density)[None, :]], axis=0
    )
    add_pieces = (
        lax.all_gather(target, "blk", axis=1, tiled=True),
        lax.all_gather(extras, "blk", axis=1, tiled=True),
    )

    def weighted_block(number, inner_sum):
        sink_part = lax.dynamic_slice_in_dim(add_pieces[0], number * block_size, block_size, 1)
        extra_part = lax.dynamic_slice_in_dim(add_pieces[1], number * block_size, block_size, 1)
        weights = kernel_block(sink_part, extra_part[0:1], anchor, anchor_half)
        return inner_sum + jnp.dot(
            extra_part[1:3],
            weights,
            precision=lax.Precision.HIGHEST,
            preferred_element_type=jnp.float32,
        )

    totals = lax.fori_loop(
        0, row_count // block_size, weighted_block, jnp.zeros((2, local_count), jnp.float32)
    )
    return finish(current_states, totals, strike)


def in_three(x):
    first = x.astype(jnp.bfloat16)
    rest = x - first.astype(jnp.float32)
    second = rest.astype(jnp.bfloat16)
    third = (rest - second.astype(jnp.float32)).astype(jnp.bfloat16)
    return first, second, third


def with_norm(pieces, norm, shift):
    rows = lax.broadcasted_iota(jnp.int32, (16, norm.shape[1]), 0)
    tile = jnp.where((rows >= 3 - shift) & (rows < 6 - shift), 1.0, 0.0)
    for k, part in enumerate(in_three(norm)):
        tile = jnp.where(rows == k + shift, part.astype(jnp.float32), tile)
    stacked = list(pieces) + [tile.astype(jnp.bfloat16)]
    height = sum(piece.shape[0] for piece in stacked)
    stacked.append(jnp.zeros((depth - height, norm.shape[1]), jnp.bfloat16))
    return jnp.concatenate(stacked, axis=0)


def source_operand(states, inverse, drift_term):
    anchor = (states + drift_term) * inverse
    half = (0.5 * log2_e) * jnp.sum(anchor * anchor, axis=0, keepdims=True)
    a1, a2, a3 = in_three(anchor * log2_e)
    return with_norm((a1, a1, a2, a1, a2, a3), -half, 0).T


def sink_operand(states, inverse):
    target = states * inverse
    half = (0.5 * log2_e) * jnp.sum(target * target, axis=0, keepdims=True)
    t1, t2, t3 = in_three(target)
    return with_norm((t1, t2, t1, t3, t2, t1), -half, 3)


def build_sources(states_refs, columns_ref, left_ref):
    inverse, drift_term = columns_ref[0], columns_ref[1]
    assets = inverse.shape[0]
    slabs = left_ref.shape[0] // lanes // len(states_refs)
    for slab in range(left_ref.shape[0] // lanes):
        row = slab % slabs * assets
        states = states_refs[slab // slabs][row : row + assets, :]
        left_ref[slab * lanes : (slab + 1) * lanes, :] = source_operand(states, inverse, drift_term)


def build_sinks(states_refs, start, columns_ref, right_ref):
    inverse = columns_ref[0]
    assets = inverse.shape[0]
    slabs = right_ref.shape[1] // lanes // len(states_refs)
    for slab in range(right_ref.shape[1] // lanes):
        row = start + slab % slabs * assets
        states = states_refs[slab // slabs][row : row + assets, :]
        right_ref[:, slab * lanes : (slab + 1) * lanes] = sink_operand(states, inverse)


def add_density(left_refs, right_ref, density_ref, first_row, base_ref=None, base_row=0):
    width = math.gcd(right_ref.shape[1], lane_tile)
    for number in range(right_ref.shape[1] // width):
        right = right_ref[:, number * width : (number + 1) * width]
        total = jnp.zeros((8, width), jnp.float32)
        for left_ref in left_refs:
            height = math.gcd(left_ref.shape[0], row_tile)
            for k in range(left_ref.shape[0] // height):
                exponent = jnp.dot(
                    left_ref[k * height : (k + 1) * height, :],
                    right,
                    preferred_element_type=jnp.float32,
                )
                total += jnp.sum(jnp.exp2(exponent).reshape(height // 8, 8, width), axis=0)
        sums = jnp.sum(total, axis=0, keepdims=True)
        for slab in range(width // lanes):
            row = number * (width // lanes) + slab
            value = sums[:, slab * lanes : (slab + 1) * lanes]
            if base_ref is not None:
                value += base_ref[base_row + row : base_row + row + 1, :]
            density_ref[first_row + row : first_row + row + 1, :] = value


def pack_kernel(*refs):
    row = 0
    for ref in refs[:-1]:
        height = min(ref.shape[0], refs[-1].shape[0] - row)
        refs[-1][row : row + height, :] = ref[0:height, :]
        row += height


def columns_kernel(table_ref, packed_ref, columns_ref):
    dates, assets = table_ref.shape[0] - 1, table_ref.shape[1]
    index = table_ref[dates : dates + 1, 0:1]
    rows = lax.broadcasted_iota(jnp.int32, (dates, assets), 0).astype(jnp.float32)
    vol_row = jnp.sum(
        jnp.where(rows == index, table_ref[0:dates, :], 0.0), axis=0, keepdims=True
    )
    square = (assets, assets)
    diagonal = lax.broadcasted_iota(jnp.int32, square, 0) == lax.broadcasted_iota(
        jnp.int32, square, 1
    )
    vol = jnp.sum(
        jnp.where(diagonal, jnp.broadcast_to(vol_row, square), 0.0), axis=1, keepdims=True
    )
    vol = jnp.broadcast_to(vol, (assets, lanes))
    columns_ref[0] = 1.0 / (vol * math.sqrt(step_years))
    columns_ref[1] = (rate_year - 0.5 * vol * vol) * step_years


def payoff_kernel(table_ref, packed_ref, payoff_ref):
    assets = table_ref.shape[1]
    strike = table_ref[table_ref.shape[0] - 1 :, 1:2]
    for slab in range(payoff_ref.shape[0]):
        prices = jnp.exp(packed_ref[slab * assets : (slab + 1) * assets, :])
        best = jnp.max(prices, axis=0, keepdims=True)
        payoff_ref[slab : slab + 1, :] = jnp.maximum(best - strike, 0.0)


def near_kernel(sources, columns_ref, first_ref, second_ref, left_ref, right_ref, density_ref):
    build_sources((first_ref, second_ref), columns_ref, left_ref)
    build_sinks((first_ref, second_ref), sources, columns_ref, right_ref)
    add_density((left_ref,), right_ref, density_ref, 0)


def near_other_kernel(columns_ref, other_ref, left_ref, right_ref, density_ref):
    build_sinks((other_ref,), 0, columns_ref, right_ref)
    add_density((left_ref,), right_ref, density_ref, 0)


def mid_kernel(sources, columns_ref, mid_ref, near_left, near_right, base, left, right, density):
    build_sinks((mid_ref,), sources, columns_ref, right)
    build_sources((mid_ref,), columns_ref, left)
    add_density((near_left, left), right, density, base.shape[0])
    add_density((left,), near_right, density, 0, base)


def far_kernel(
    sources,
    columns_ref,
    far_ref,
    near_left,
    mid_left,
    near_right,
    mid_right,
    base,
    left,
    right,
    density,
):
    near_slabs = near_right.shape[1] // lanes
    build_sinks((far_ref,), sources, columns_ref, right)
    build_sources((far_ref,), columns_ref, left)
    add_density((near_left, mid_left, left), right, density, base.shape[0])
    add_density((left,), near_right, density, 0, base)
    add_density((left,), mid_right, density, near_slabs, base, near_slabs)


def far_other_kernel(
    columns_ref,
    other_ref,
    near_left,
    mid_left,
    far_left,
    near_right,
    base,
    own_density,
    right,
    density,
):
    rows = own_density.shape[0]
    density[0:rows, :] = own_density[...]
    add_density((mid_left, far_left), near_right, density, rows, base)
    build_sinks((other_ref,), 0, columns_ref, right)
    add_density((near_left, mid_left, far_left), right, density, rows + base.shape[0])


def matrix_kernel(left_ref, *refs):
    matrix_ref = refs[-1]
    place = 0
    for right_ref in refs[:-1]:
        width = math.gcd(right_ref.shape[1], lane_tile)
        for number in range(right_ref.shape[1] // width):
            matrix_ref[:, place : place + width] = jnp.exp2(
                jnp.dot(
                    left_ref[...],
                    right_ref[:, number * width : (number + 1) * width],
                    preferred_element_type=jnp.float32,
                )
            )
            place += width


def weight_kernel(assets, matrix_ref, density_ref, received_ref, *refs):
    *values_refs, payoff_ref, continuation_ref, node_ref, ratio_ref = refs
    slabs = density_ref.shape[0]
    half = slabs // 2
    inverse = 1.0 / jnp.concatenate(
        [
            density_ref[:half, :] + received_ref[half:, :],
            density_ref[half:, :] + received_ref[:half, :],
        ],
        axis=0,
    )
    ratio_ref[1] = inverse
    row = 0
    for k, values_ref in enumerate(values_refs):
        rows_per_slab = 2 * assets + 1 if k < 4 else assets + 1
        count = values_ref.shape[0] // rows_per_slab
        values = values_ref[values_ref.shape[0] - count :, :]
        ratio_ref[0, row : row + count, :] = values * inverse[row : row + count]
        row += count
    count = matrix_ref.shape[0]
    height = math.gcd(count, 64)
    sums = []
    for k in range(count // height):
        weighted = jnp.zeros((height, lanes), jnp.float32)
        mass = jnp.zeros((height, lanes), jnp.float32)
        for slab in range(slabs):
            piece = matrix_ref[k * height : (k + 1) * height, slab * lanes : (slab + 1) * lanes]
            weighted += piece * ratio_ref[0, slab : slab + 1, :]
            mass += piece * ratio_ref[1, slab : slab + 1, :]
        sums.append((weighted, mass))
    per_slab = lanes // height
    for slab in range(count // lanes):
        group = sums[slab * per_slab : (slab + 1) * per_slab]
        weighted, mass = (
            jnp.sum(jnp.concatenate([pair[k] for pair in group], axis=0).T, axis=0, keepdims=True)
            for k in range(2)
        )
        continuation = math.exp(-rate_year * step_years) * weighted / mass
        continuation_ref[slab : slab + 1, :] = continuation
        node_ref[slab : slab + 1, :] = jnp.maximum(payoff_ref[slab : slab + 1, :], continuation)


vmem = pl.BlockSpec(memory_space=pltpu.VMEM)


def local_call(kernel, in_specs, out_shapes, matmul_pairs=0, scratch_shapes=()):
    cost = pl.CostEstimate(
        flops=2 * depth * matmul_pairs, transcendentals=matmul_pairs, bytes_accessed=0
    )
    return pl.pallas_call(
        kernel,
        out_shape=out_shapes,
        in_specs=in_specs,
        out_specs=[vmem] * len(out_shapes),
        scratch_shapes=scratch_shapes,
        cost_estimate=cost,
        compiler_params=pltpu.CompilerParams(vmem_limit_bytes=vmem_grant),
    )


def doubled_body(blk_size, current_states, next_states, next_values, vol_table, date_index, strike):
    assets, count = current_states.shape
    own_slabs = count // lanes

    def across(array, mask):
        return lax.ppermute(array, "blk", [(i, i ^ mask) for i in range(blk_size)])

    def floats(*shape):
        return jax.ShapeDtypeStruct(shape, jnp.float32)

    def halves(*shape):
        return jax.ShapeDtypeStruct(shape, jnp.bfloat16)

    pieces = [
        part[:, slab * lanes : (slab + 1) * lanes]
        for part in (current_states, next_states)
        for slab in range(own_slabs)
    ]
    rows = lax.pad(
        next_values.reshape(own_slabs, lanes), jnp.float32(0), ((0, assets - own_slabs, 0), (0, 0, 0))
    )
    tile_rows = lax.broadcasted_iota(jnp.int32, rows.shape, 0)
    pieces.append(jnp.where(tile_rows < own_slabs, rows, pieces[0]))
    (packed,) = local_call(
        pack_kernel, [vmem] * len(pieces), [floats((2 * assets + 1) * own_slabs, lanes)]
    )(*pieces)
    places = lax.broadcasted_iota(jnp.int32, (1, assets), 1)
    last = jnp.where(places == 0, date_index.astype(jnp.float32), jnp.where(places == 1, strike, 0.0))
    table = jnp.concatenate([vol_table, last], axis=0)
    (columns,) = local_call(columns_kernel, [vmem, vmem], [floats(2, assets, lanes)])(table, packed)

    slabs = own_slabs
    mask = blk_size // 2
    while mask > 4:
        received = across(packed, mask)
        cuts = (0, assets * slabs, 2 * assets * slabs, (2 * assets + 1) * slabs)
        packed = jnp.concatenate(
            [part[a:b] for a, b in zip(cuts, cuts[1:]) for part in (packed, received)], axis=0
        )
        if slabs == own_slabs:
            packed, columns = lax.optimization_barrier((packed, columns))
        slabs *= 2
        mask //= 2
    sources = assets * slabs
    near = across(packed, 4)
    mid = across(packed, 6)
    far = across(packed, 2)
    (payoff,) = local_call(payoff_kernel, [vmem, vmem], [floats(own_slabs, lanes)])(table, packed)
    nodes = slabs * lanes
    targets, values = slice(sources, 2 * sources), slice(2 * sources, None)

    def sinks(first, second):
        return jnp.concatenate([first[targets], second[targets], first[values], second[values]])

    near_other = across(sinks(packed, near), 1)
    left, right, base = local_call(
        functools.partial(near_kernel, sources),
        [vmem] * 3,
        [halves(2 * nodes, depth), halves(depth, 2 * nodes), floats(2 * slabs, lanes)],
        4 * nodes * nodes,
    )(columns, packed, near)
    other_right, other_base = local_call(
        near_other_kernel,
        [vmem] * 3,
        [halves(depth, 2 * nodes), floats(2 * slabs, lanes)],
        4 * nodes * nodes,
    )(columns, near_other, left)
    mid_left, mid_right, mid_base = local_call(
        functools.partial(mid_kernel, sources),
        [vmem] * 5,
        [halves(nodes, depth), halves(depth, nodes), floats(3 * slabs, lanes)],
        5 * nodes * nodes,
    )(columns, mid, left, right, base)
    far_other = across(sinks(mid, far), 1)
    far_left, far_right, density = local_call(
        functools.partial(far_kernel, sources),
        [vmem] * 7,
        [halves(nodes, depth), halves(depth, nodes), floats(4 * slabs, lanes)],
        7 * nodes * nodes,
    )(columns, far, left, mid_left, right, mid_right, mid_base)
    far_other_right, density = local_call(
        far_other_kernel,
        [vmem] * 8,
        [halves(depth, 2 * nodes), floats(8 * slabs, lanes)],
        12 * nodes * nodes,
    )(columns, far_other, left, mid_left, far_left, other_right, other_base, density)
    received = across(density, 1)
    (matrix,) = local_call(
        matrix_kernel, [vmem] * 6, [floats(count, 8 * nodes)], 8 * count * nodes
    )(left[:count], right, mid_right, far_right, other_right, far_other_right)
    continuation, node_value = local_call(
        functools.partial(weight_kernel, assets),
        [vmem] * 10,
        [floats(own_slabs, lanes)] * 2,
        scratch_shapes=[pltpu.VMEM((2, 8 * slabs, lanes), jnp.float32)],
    )(
        matrix,
        density,
        received,
        packed,
        near,
        mid,
        far,
        near_other,
        far_other,
        payoff,
    )
    return continuation.reshape(count), node_value.reshape(count)


def solution(mesh):
    blk_size = mesh.shape["blk"]
    placed = (
        P(None, ("groups", "blk")),
        P(None, ("groups", "blk")),
        P(("groups", "blk")),
        P(),
        P(),
        P(),
    )
    doubled = blk_size in (16, 32)
    return jax.shard_map(
        functools.partial(doubled_body, blk_size) if doubled else gathered_body,
        mesh=mesh,
        in_specs=placed,
        out_specs=(P(("groups", "blk")), P(("groups", "blk"))),
        check_vma=False,
    )
```
